256 devices in a mesh: chain: 8 (over x, core), blk: 32 (over z, y).
Axes of the slice: x: 4, y: 4, z: 8, core: 2. Of those that a mesh axis runs over, the one named last changes fastest.
Arguments:
- schur: bfloat16 [16384, 2048], P(('chain', 'blk')), as said below
- coupling: bfloat16 [16384, 2048], P(('chain', 'blk')), may hold values from -0.0625 to 0.0625
- next_diag: float32 [16384, 2048], P(('chain', 'blk')), as said below
Outputs:
- factor: float32 [16384, 2048], P(('chain', 'blk'))
- next_schur: float32 [16384, 2048], P(('chain', 'blk'))
The draws below stay inside these ranges and needn't reach their ends.
Inputs may be any that keep to these rules, and one draw needn't show every extreme that they name: `schur`: every slab's block is symmetric positive definite. `next_diag`: every slab's block is symmetric positive definite.
All inputs are finite; a program needn't handle non-finite values.
Results may differ from the reference program's by a relative error of at most 0.0034.
Values may be sent and summed in bfloat16 or wider, within the bound.
No kernel may reach another device: no remote copies, remote signals or barrier semaphores. Data moves between devices by JAX's collectives and lax.ppermute only.
A program may use at most 128 MiB of HBM per device.

```python
import jax
import jax.numpy as jnp
from jax import lax

NB = 2048
SLABS = 8


def spd_slabs(key, floor_value):
    noise_key, shift_key = jax.random.split(key)
    raw = jax.random.normal(noise_key, (SLABS, NB, NB), jnp.float32)
    floor_part = floor_value * (1.0 + 0.5 * jax.random.uniform(shift_key, (SLABS, NB), jnp.float32))
    gram = jnp.einsum('sij,skj->sik', raw, raw, precision=lax.Precision.HIGHEST) / jnp.float32(NB)
    matrix = gram + floor_part[:, :, None] * jnp.eye(NB, dtype=jnp.float32)[None, :, :]
    return matrix.reshape(SLABS * NB, NB)


def draw_schur(key, part):
    return spd_slabs(jax.random.fold_in(key, 11), 0.02).astype(jnp.bfloat16)


def draw_next_diag(key, part):
    return spd_slabs(jax.random.fold_in(key, 23), 2.0)


def steps_of(own_key, shape, pieces, least, largest):
    level, own = 1.0, jax.random.fold_in(own_key, 6)
    for axis_at, parts in pieces:
        steps = jnp.exp(jax.random.uniform(jax.random.fold_in(own, axis_at), (parts,), jnp.float32, least / len(pieces), largest / len(pieces)))
        level = level * jnp.repeat(steps, shape[axis_at] // parts).reshape([-1 if axis == axis_at else 1 for axis in range(len(shape))])
    return level


def normal_values(key, dims, spread, most, shards=(), held_as=jnp.bfloat16):
    gain = steps_of(key, dims, shards, -0.22, 0.18) if shards else 1.0
    values = jax.random.normal(key, dims, jnp.float32) * spread * gain
    return jnp.minimum(jnp.maximum(values, -most), most).astype(held_as)


def setup_inputs(seed: int = 0) -> dict:
    keys = jax.random.split(jax.random.key(seed), 4)
    return {
        "schur": draw_schur(jax.random.fold_in(keys[3], 71), 0),
        "coupling": normal_values(keys[1], (SLABS * NB, NB), (4 * NB) ** -0.5, 0.0625, ((0, 256),)),
        "next_diag": draw_next_diag(jax.random.fold_in(keys[3], 71), 0),
    }


def factor_slab(blocks_pair):
    diag_block, couple_block = blocks_pair
    lower = jnp.linalg.cholesky(diag_block.astype(jnp.float32))
    solved = lax.linalg.triangular_solve(lower, couple_block.astype(jnp.float32).T, left_side=True, lower=True).astype(jnp.bfloat16)
    update = jnp.dot(solved.T.astype(jnp.float32), solved.astype(jnp.float32), preferred_element_type=jnp.float32)
    return (lower, update)

def reference(schur, coupling, next_diag):
    blocks = schur.reshape(SLABS, NB, NB)
    couple = coupling.reshape(SLABS, NB, NB)
    factors, updates = lax.map(factor_slab, (blocks, couple))
    shifted = jnp.concatenate([jnp.zeros((1, NB, NB), jnp.float32), updates[:-1]], axis=0)
    fresh = next_diag.reshape(SLABS, NB, NB) - shifted
    return (factors.reshape(SLABS * NB, NB), fresh.reshape(SLABS * NB, NB))
```

```python
import jax
import jax.numpy as jnp
from jax import lax
from jax.experimental import pallas as pl
from jax.experimental.pallas import tpu as pltpu
from jax.sharding import PartitionSpec as P

F32, BF16 = jnp.float32, jnp.bfloat16
N = 2048
W = 256
PANELS = N // W
VMEM_LIMIT = 62 * 1024 * 1024

def split(x):
    hi = x.astype(BF16)
    return hi, (x - hi.astype(F32)).astype(BF16)

def dot(a, b, ca, cb):
    return lax.dot_general(a, b, (((ca,), (cb,)), ((), ())), preferred_element_type=F32)

def dot3(a, b, ca, cb):
    return dot(a[0], b[0], ca, cb) + (dot(a[0], b[1], ca, cb) + dot(a[1], b[0], ca, cb))

def row_of(x, s):
    return jnp.broadcast_to(x[s : s + 1, :], (8, 128))

def lane_of(x, c):
    return jnp.broadcast_to(x[:, c : c + 1], (8, 128))

def inverse_factor(read, write):
    lane = lax.broadcasted_iota(jnp.int32, (8, 128), 1)
    strips = [read(k) for k in range(16)]
    for k in range(16):
        base = 8 * k
        inside = (lane >= base) & (lane < base + 8)
        cols = {q: [lane_of(strips[q], base + c) for c in range(8)] for q in range(k, 16)}
        for q in range(k + 1, 16):
            strips[q] = jnp.where(inside, 0.0, strips[q])
        rows = [jnp.where(inside, jnp.where(lane == base + s, 1.0, 0.0), row_of(strips[k], s)) for s in range(8)]
        own = cols[k]
        nxt = cols[k + 1] if k < 15 else None
        scale, factor = [], {}
        for c in range(8):
            pivot = row_of(own[c], c)
            r = 1.0 / pivot
            scale.append(r)
            write(base + c, jnp.where(lane < base + 8, rows[c] * lax.rsqrt(pivot), 0.0)[:1, :])
            for s in range(c + 1, 8):
                f = row_of(own[c], s) * r
                factor[s, c] = f
                own[s] = own[s] - own[c] * f
                rows[s] = rows[s] - rows[c] * f
                if nxt is not None:
                    nxt[s] = nxt[s] - nxt[c] * f
            if nxt is not None:
                strips[k + 1] = strips[k + 1] - (nxt[c] * r) * rows[c]
        if k < 14:
            solved = [None] * 8
            for s in range(7, -1, -1):
                v = rows[s] * scale[s]
                for t in range(s + 1, 8):
                    v = v - factor[t, s] * solved[t]
                solved[s] = v
            for q in range(k + 2, 16):
                for c in range(8):
                    strips[q] = strips[q] - cols[q][c] * solved[c]


def rows_at(start, size):
    return pl.ds(pl.multiple_of(start, size), size)


def factor_kernel(where_ref, g_ref, hi_ref, lo_ref, thi_ref, tlo_ref, f_ref, a_ref, p_ref, d_ref, t_ref):
    for i in range(16):
        for j in range(i + 1):
            gap = i - j
            if gap <= 8:
                block = g_ref[128 * i : 128 * i + 128, 128 * (8 - gap) : 128 * (9 - gap)]
            else:
                block = g_ref[128 * j : 128 * j + 128, 128 * (gap - 8) : 128 * (gap - 7)].astype(F32).T.astype(BF16)
            a_ref[128 * i : 128 * i + 128, 128 * j : 128 * j + 128] = block
        if i % 2 == 0:
            a_ref[128 * i : 128 * i + 128, 128 * i + 128 : 128 * i + 256] = jnp.zeros((128, 128), BF16)

    def panel(p, carry):
        cols = rows_at(p * W, W)

        def update(t, carry):
            rows = rows_at(t * W, W)
            p_ref[rows, :] = a_ref[rows, cols].astype(F32)

            def past(i, carry):
                old = rows_at(i * W, W)
                p_ref[rows, :] -= dot3(
                    (hi_ref[rows, old], lo_ref[rows, old]), (hi_ref[cols, old], lo_ref[cols, old]), 1, 1
                )
                return carry

            return lax.fori_loop(0, p, past, carry)

        lax.fori_loop(p, PANELS, update, 0)
        top = rows_at(p * W, 128)
        low = rows_at(p * W + 128, 128)

        def half(h, carry):
            @pl.when(h == 0)
            def _():
                d_ref[...] = p_ref[top, 0:128]

            @pl.when(h == 1)
            def _():
                below = dot3(split(p_ref[low, 0:128]), split(t_ref[0]), 1, 1)
                pair = split(below)
                d_ref[...] = p_ref[low, 128:256] - dot3(pair, pair, 1, 1)
                t_ref[2] = dot3(pair, split(t_ref[0]), 1, 0)

            def write(r, v):
                t_ref[h, r : r + 1, :] = v

            inverse_factor(lambda k: d_ref[8 * k : 8 * k + 8, :], write)
            return carry

        lax.fori_loop(0, 2, half, 0)
        corner = split(t_ref[1])
        blocks = (split(t_ref[0]), split(-dot3(corner, split(t_ref[2]), 1, 0)), corner)
        for part, out in ((0, thi_ref), (1, tlo_ref)):
            out[top, 0:128] = blocks[0][part]
            out[top, 128:256] = jnp.zeros((128, 128), BF16)
            out[low, 0:128] = blocks[1][part]
            out[low, 128:256] = blocks[2][part]

        def scale(t, carry):
            rows = rows_at(t * W, W)
            new = split(dot3(split(p_ref[rows, :]), (thi_ref[cols, :], tlo_ref[cols, :]), 1, 1))
            hi_ref[rows, cols] = new[0]
            lo_ref[rows, cols] = new[1]
            return carry

        return lax.fori_loop(p, PANELS, scale, carry)

    lax.fori_loop(0, PANELS, panel, 0)
    first = where_ref[0] * 64
    mine = rows_at(first, 64)
    keep = lax.broadcasted_iota(jnp.int32, (64, N), 1) <= lax.broadcasted_iota(jnp.int32, (64, N), 0) + first
    f_ref[...] = jnp.where(keep, hi_ref[mine, :].astype(F32) + lo_ref[mine, :].astype(F32), 0.0)


def solve_kernel(where_ref, cr_ref, ck_ref, hi_ref, lo_ref, thi_ref, tlo_ref, *refs):
    u_refs, (yhi_ref, ylo_ref, p_ref, u_ref) = refs[:8], refs[8:]

    def panel(p, carry):
        cols = rows_at(p * W, W)
        p_ref[0:512, :] = cr_ref[:, cols].astype(F32)
        p_ref[512:768, :] = ck_ref[:, cols].astype(F32)

        def past(i, carry):
            old = rows_at(i * W, W)
            p_ref[...] -= dot3((yhi_ref[:, old], ylo_ref[:, old]), (hi_ref[cols, old], lo_ref[cols, old]), 1, 1)
            return carry

        lax.fori_loop(0, p, past, 0)
        new = split(dot3(split(p_ref[...]), (thi_ref[cols, :], tlo_ref[cols, :]), 1, 1))
        yhi_ref[:, cols] = new[0]
        ylo_ref[:, cols] = new[1]
        return carry

    lax.fori_loop(0, PANELS, panel, 0)
    u_ref[...] = dot(yhi_ref[0:512, :], yhi_ref[512:768, :], 1, 1).astype(BF16)
    for m in range(8):
        u_refs[m][...] = u_ref[rows_at(lax.rem(where_ref[0] + m, 8) * 64, 64), :]


def finish_kernel(where_ref, nd_ref, *refs):
    parts, out_ref = refs[:8], refs[8]
    for m in range(8):
        cols = rows_at(lax.rem(where_ref[0] + 8 - m, 8) * W, W)
        out_ref[:, cols] = nd_ref[:, cols] - parts[m][...].astype(F32)


def vmem(count):
    return [pl.BlockSpec(memory_space=pltpu.VMEM)] * count


def smem():
    return [pl.BlockSpec(memory_space=pltpu.SMEM)]


def shape(dims, dtype):
    return jax.ShapeDtypeStruct(dims, dtype)


def cost(flops, moved):
    return pl.CostEstimate(flops=flops, bytes_accessed=moved, transcendentals=0)


def local(schur, coupling, next_diag):
    params = pltpu.CompilerParams(vmem_limit_bytes=VMEM_LIMIT)
    index = lax.axis_index("blk")
    blk = index.astype(jnp.int32).reshape(1)
    high = blk // 4
    start = 128 * ((index // 2 + 8) % 16)
    half = lax.dynamic_slice_in_dim(jnp.concatenate([schur, schur[:, :1024]], axis=1), start, 1152, 1)
    gathered = lax.all_gather(half, "blk", axis=0, tiled=True)
    lines_z = [[4 * z + y for z in range(8)] for y in range(4)]
    lines_y = [[4 * z + y for y in range(4)] for z in range(8)]
    c_rows = lax.all_gather(coupling, "blk", axis=0, tiled=True, axis_index_groups=lines_z)
    c_cols = lax.all_gather(coupling, "blk", axis=0, tiled=True, axis_index_groups=lines_y)
    hi, lo, thi, tlo, mine = pl.pallas_call(
        factor_kernel,
        out_shape=[shape((N, N), BF16), shape((N, N), BF16), shape((N, W), BF16), shape((N, W), BF16), shape((64, N), F32)],
        in_specs=smem() + vmem(1),
        out_specs=vmem(5),
        scratch_shapes=[
            pltpu.VMEM((N, N), BF16),
            pltpu.VMEM((N, W), F32),
            pltpu.VMEM((128, 128), F32),
            pltpu.VMEM((3, 128, 128), F32),
        ],
        compiler_params=params,
        cost_estimate=cost(60_000_000_000, 24_000_000),
    )(blk, gathered)
    parts = pl.pallas_call(
        solve_kernel,
        out_shape=[shape((64, W), BF16)] * 8,
        in_specs=smem() + vmem(6),
        out_specs=vmem(8),
        scratch_shapes=[
            pltpu.VMEM((768, N), BF16),
            pltpu.VMEM((768, N), BF16),
            pltpu.VMEM((768, W), F32),
            pltpu.VMEM((512, W), BF16),
        ],
        compiler_params=params,
        cost_estimate=cost(12_000_000_000, 24_000_000),
    )(high, c_rows, c_cols, hi, lo, thi, tlo)
    arrived = []
    for m in range(8):
        pairs = [
            (32 * s + 4 * z + y, 32 * (s + 1) + 4 * ((z + m) % 8) + y)
            for s in range(7)
            for z in range(8)
            for y in range(4)
        ]
        arrived.append(lax.ppermute(parts[m], ("chain", "blk"), pairs))
    fresh = pl.pallas_call(
        finish_kernel,
        out_shape=shape((64, N), F32),
        in_specs=smem() + vmem(9),
        out_specs=pl.BlockSpec(memory_space=pltpu.VMEM),
        cost_estimate=cost(200_000, 1_400_000),
    )(high, next_diag, *arrived)
    return (mine, fresh)


def solution(mesh):
    placed = P(("chain", "blk"), None)
    return jax.shard_map(
        local, mesh=mesh, in_specs=(placed, placed, placed), out_specs=(placed, placed), check_vma=False
    )
```

```python
import jax
import jax.numpy as jnp
from jax import lax
from jax.experimental import pallas as pl
from jax.experimental.pallas import tpu as pltpu
from jax.sharding import PartitionSpec as P

F32, BF16 = jnp.float32, jnp.bfloat16
N = 2048
W = 256
PANELS = N // W
SPLIT = 512
VMEM_LIMIT = 62 * 1024 * 1024

def split(x):
    hi = x.astype(BF16)
    return hi, (x - hi.astype(F32)).astype(BF16)

def dot(a, b, ca, cb):
    return lax.dot_general(a, b, (((ca,), (cb,)), ((), ())), preferred_element_type=F32)

def dot3(a, b, ca, cb):
    return dot(a[0], b[0], ca, cb) + (dot(a[0], b[1], ca, cb) + dot(a[1], b[0], ca, cb))

def row_of(x, s):
    return jnp.broadcast_to(x[s : s + 1, :], (8, 128))

def lane_of(x, c):
    return jnp.broadcast_to(x[:, c : c + 1], (8, 128))

def inverse_factor(read, write, one):
    lane = lax.broadcasted_iota(jnp.int32, (8, 128), 1)
    strips = [read(k) for k in range(16)]
    for k in range(16):
        base = 8 * k
        inside = (lane >= base) & (lane < base + 8)
        cols = {q: [lane_of(strips[q], base + c) for c in range(8)] for q in range(k, 16)}
        for q in range(k + 1, 16):
            strips[q] = jnp.where(inside, 0.0, strips[q])
        rows = [jnp.where(inside, jnp.where(lane == base + s, 1.0, 0.0), row_of(strips[k], s)) for s in range(8)]
        own = [x * one for x in cols[k]]
        nxt = cols[k + 1] if k < 15 else None
        scale, factor = [], {}
        for c in range(8):
            pivot = row_of(own[c], c)
            r = 1.0 / pivot
            scale.append(r)
            write(base + c, jnp.where(lane < base + 8, rows[c] * lax.rsqrt(pivot), 0.0)[:1, :])
            for s in range(c + 1, 8):
                f = row_of(own[c], s) * r
                factor[s, c] = f
                own[s] = own[s] - own[c] * f
                rows[s] = rows[s] - rows[c] * f
                if nxt is not None:
                    nxt[s] = nxt[s] - nxt[c] * f
            if nxt is not None:
                strips[k + 1] = strips[k + 1] - (nxt[c] * r) * rows[c]
        if k < 14:
            solved = [None] * 8
            for s in range(7, -1, -1):
                v = rows[s] * scale[s]
                for t in range(s + 1, 8):
                    v = v - factor[t, s] * solved[t]
                solved[s] = v
            for q in range(k + 2, 16):
                for c in range(8):
                    strips[q] = strips[q] - cols[q][c] * solved[c]


def rows_at(start, size):
    return pl.ds(pl.multiple_of(start, size), size)


def factor_kernel(where_ref, one_ref, *refs):
    narrow_refs, wide_refs = refs[:9], refs[9:14]
    hi_ref, lo_ref, thi_ref, tlo_ref, f_ref, a_ref, p_ref, d_ref, t_ref, g_ref = refs[14:]
    z, y = where_ref[0] // 4, lax.rem(where_ref[0], 4)

    def place(ref, at, steps_z, steps_y, first, last):
        to = 4 * lax.rem(z + steps_z + 8, 8) + lax.rem(y + steps_y + 4, 4)
        g_ref[rows_at(to * 64, 64), first:last] = ref[64 * at : 64 * at + 64, :]

    for ref, dz, slots in zip(narrow_refs, (0, -1, 1, -2, 2, -3, 3, 4, 4), [(0, 1, 2, 3)] * 7 + [(0, 1), (2, 3)]):
        for at, slot in enumerate(slots):
            place(ref, at, dz, (0, -1, 1, 2)[slot], 0, SPLIT)
    for ref, dy, slots in zip(wide_refs, (0, -1, 1, 2, 2), [range(8)] * 3 + [range(4), range(4, 8)]):
        for at, slot in enumerate(slots):
            place(ref, at, (0, -1, 1, -2, 2, -3, 3, 4)[slot], dy, SPLIT, 1152)
    for i in range(16):
        for j in range(i + 1):
            gap = i - j
            if gap <= 8:
                block = g_ref[128 * i : 128 * i + 128, 128 * (8 - gap) : 128 * (9 - gap)]
            else:
                block = g_ref[128 * j : 128 * j + 128, 128 * (gap - 8) : 128 * (gap - 7)].astype(F32).T.astype(BF16)
            a_ref[128 * i : 128 * i + 128, 128 * j : 128 * j + 128] = block
        if i % 2 == 0:
            a_ref[128 * i : 128 * i + 128, 128 * i + 128 : 128 * i + 256] = jnp.zeros((128, 128), BF16)

    def panel(p, carry):
        cols = rows_at(p * W, W)

        def update(t, carry):
            rows = rows_at(t * W, W)
            p_ref[rows, :] = a_ref[rows, cols].astype(F32)

            def past(i, carry):
                old = rows_at(i * W, W)
                p_ref[rows, :] -= dot3(
                    (hi_ref[rows, old], lo_ref[rows, old]), (hi_ref[cols, old], lo_ref[cols, old]), 1, 1
                )
                return carry

            return lax.fori_loop(0, p, past, carry)

        lax.fori_loop(p, PANELS, update, 0)
        top = rows_at(p * W, 128)
        low = rows_at(p * W + 128, 128)

        def half(h, carry):
            @pl.when(h == 0)
            def _():
                d_ref[...] = p_ref[top, 0:128]

            @pl.when(h == 1)
            def _():
                below = dot3(split(p_ref[low, 0:128]), split(t_ref[0]), 1, 1)
                pair = split(below)
                d_ref[...] = p_ref[low, 128:256] - dot3(pair, pair, 1, 1)
                t_ref[2] = dot3(pair, split(t_ref[0]), 1, 0)

            def write(r, v):
                t_ref[h, r : r + 1, :] = v

            inverse_factor(lambda k: d_ref[8 * k : 8 * k + 8, :], write, one_ref[...])
            return carry

        lax.fori_loop(0, 2, half, 0)
        corner = split(t_ref[1])
        blocks = (split(t_ref[0]), split(-dot3(corner, split(t_ref[2]), 1, 0)), corner)
        for part, out in ((0, thi_ref), (1, tlo_ref)):
            out[top, 0:128] = blocks[0][part]
            out[top, 128:256] = jnp.zeros((128, 128), BF16)
            out[low, 0:128] = blocks[1][part]
            out[low, 128:256] = blocks[2][part]

        def scale(t, carry):
            rows = rows_at(t * W, W)
            new = split(dot3(split(p_ref[rows, :]), (thi_ref[cols, :], tlo_ref[cols, :]), 1, 1))
            hi_ref[rows, cols] = new[0]
            lo_ref[rows, cols] = new[1]
            return carry

        return lax.fori_loop(p, PANELS, scale, carry)

    lax.fori_loop(0, PANELS, panel, 0)
    first = where_ref[0] * 64
    mine = rows_at(first, 64)
    keep = lax.broadcasted_iota(jnp.int32, (64, N), 1) <= lax.broadcasted_iota(jnp.int32, (64, N), 0) + first
    f_ref[...] = jnp.where(keep, hi_ref[mine, :].astype(F32) + lo_ref[mine, :].astype(F32), 0.0)


def solve_kernel(ck_ref, cr_ref, hi_ref, lo_ref, thi_ref, tlo_ref, u_ref, yhi_ref, ylo_ref, p_ref):
    def panel(p, carry):
        cols = rows_at(p * W, W)
        p_ref[0:512, :] = ck_ref[:, cols].astype(F32)
        p_ref[512:768, :] = cr_ref[:, cols].astype(F32)

        def past(i, carry):
            old = rows_at(i * W, W)
            p_ref[...] -= dot3((yhi_ref[:, old], ylo_ref[:, old]), (hi_ref[cols, old], lo_ref[cols, old]), 1, 1)
            return carry

        lax.fori_loop(0, p, past, 0)
        new = split(dot3(split(p_ref[...]), (thi_ref[cols, :], tlo_ref[cols, :]), 1, 1))
        yhi_ref[:, cols] = new[0]
        ylo_ref[:, cols] = new[1]
        return carry

    lax.fori_loop(0, PANELS, panel, 0)
    u_ref[...] = dot(yhi_ref[512:768, :], yhi_ref[0:512, :], 1, 1).astype(BF16)


def finish_kernel(nd_ref, part_ref, out_ref):
    for q in range(16):
        left = 128 * (q % 2)
        lanes = slice(64 * (q // 2), 64 * (q // 2) + 64)
        pair = [part_ref[left + 64 * e : left + 64 * e + 64, lanes].astype(F32) for e in range(2)]
        cols = slice(128 * q, 128 * q + 128)
        out_ref[:, cols] = nd_ref[:, cols] - jnp.concatenate(pair, axis=1)


def vmem(count):
    return [pl.BlockSpec(memory_space=pltpu.VMEM)] * count


def smem():
    return [pl.BlockSpec(memory_space=pltpu.SMEM)]


def shape(dims, dtype):
    return jax.ShapeDtypeStruct(dims, dtype)


def cost(flops, moved):
    return pl.CostEstimate(flops=flops, bytes_accessed=moved, transcendentals=0)


def shifted(value, by_z, by_y):
    pairs = [(4 * z + y, 4 * ((z + by_z) % 8) + (y + by_y) % 4) for z in range(8) for y in range(4)]
    return lax.ppermute(value, "blk", pairs)


def around(value, steps, by_z, by_y):
    up = down = value
    got = []
    for _ in range(steps - 1):
        up, down = shifted(up, by_z, by_y), shifted(down, -by_z, -by_y)
        got += [up, down]
    half = value.shape[0] // 2
    return got + [shifted(up[:half], by_z, by_y), shifted(down[half:], -by_z, -by_y)]


def local(schur, coupling, next_diag):
    params = pltpu.CompilerParams(vmem_limit_bytes=VMEM_LIMIT)
    index = lax.axis_index("blk")
    blk = index.astype(jnp.int32).reshape(1)
    start = 128 * ((index // 2 + 8) % 16)
    half = lax.dynamic_slice_in_dim(jnp.concatenate([schur, schur[:, :1024]], axis=1), start, 1152, 1)
    narrow, wide = half[:, :SPLIT], half[:, SPLIT:]
    wide = jnp.concatenate([wide] + around(wide, 4, 1, 0), axis=0)
    narrow = jnp.concatenate([narrow] + around(narrow, 2, 0, 1), axis=0)
    narrow_parts = [narrow] + around(narrow, 4, 1, 0)
    wide_parts = [wide] + around(wide, 2, 0, 1)
    pieces = lax.optimization_barrier(tuple(narrow_parts + wide_parts) + (coupling,))
    coupling = pieces[-1]
    lines_z = [[4 * z + y for z in range(8)] for y in range(4)]
    lines_y = [[4 * z + y for y in range(4)] for z in range(8)]
    c_cols = lax.all_gather(coupling, "blk", axis=0, tiled=True, axis_index_groups=lines_z)
    c_rows = lax.all_gather(coupling, "blk", axis=0, tiled=True, axis_index_groups=lines_y)
    hi, lo, thi, tlo, mine = pl.pallas_call(
        factor_kernel,
        out_shape=[shape((N, N), BF16), shape((N, N), BF16), shape((N, W), BF16), shape((N, W), BF16), shape((64, N), F32)],
        in_specs=smem() + vmem(15),
        out_specs=vmem(5),
        scratch_shapes=[
            pltpu.VMEM((N, N), BF16),
            pltpu.VMEM((N, W), F32),
            pltpu.VMEM((128, 128), F32),
            pltpu.VMEM((3, 128, 128), F32),
            pltpu.VMEM((N, 1152), BF16),
        ],
        compiler_params=params,
        cost_estimate=cost(60_000_000_000, 24_000_000),
    )(blk, jnp.ones((8, 128), F32), *pieces[:-1])
    part = pl.pallas_call(
        solve_kernel,
        out_shape=shape((W, 512), BF16),
        in_specs=vmem(6),
        out_specs=pl.BlockSpec(memory_space=pltpu.VMEM),
        scratch_shapes=[
            pltpu.VMEM((768, N), BF16),
            pltpu.VMEM((768, N), BF16),
            pltpu.VMEM((768, W), F32),
        ],
        compiler_params=params,
        cost_estimate=cost(12_000_000_000, 24_000_000),
    )(c_cols, c_rows, hi, lo, thi, tlo)
    part = lax.all_to_all(part, "blk", 0, 0, axis_index_groups=lines_y, tiled=True)
    count = lax.axis_size("chain")
    part = lax.ppermute(part, "chain", [(s, s + 1) for s in range(count - 1)])
    fresh = pl.pallas_call(
        finish_kernel,
        out_shape=shape((64, N), F32),
        in_specs=vmem(2),
        out_specs=pl.BlockSpec(memory_space=pltpu.VMEM),
        cost_estimate=cost(200_000, 1_400_000),
    )(next_diag, part)
    return (mine, fresh)


def solution(mesh):
    placed = P(("chain", "blk"), None)
    return jax.shard_map(
        local, mesh=mesh, in_specs=(placed, placed, placed), out_specs=(placed, placed), check_vma=False
    )
```

```python
import jax
import jax.numpy as jnp
from jax import lax
from jax.experimental import pallas as pl
from jax.experimental.pallas import tpu as pltpu
from jax.sharding import PartitionSpec as P

F32, BF16 = jnp.float32, jnp.bfloat16
N = 2048
W = 256
PANELS = N // W
SLOTS = 13
VMEM_LIMIT = 62 * 1024 * 1024


def split(x):
    hi = x.astype(BF16)
    return hi, (x - hi.astype(F32)).astype(BF16)


def dot(a, b, ca, cb):
    return lax.dot_general(a, b, (((ca,), (cb,)), ((), ())), preferred_element_type=F32)


def dot3(a, b, ca, cb):
    left = jnp.concatenate([a[0], a[0], a[1]], axis=ca)
    right = jnp.concatenate([b[0], b[1], b[0]], axis=cb)
    return dot(left, right, ca, cb)


def row_of(x, s):
    return jnp.broadcast_to(x[s : s + 1, :], (8, 128))


def lane_of(x, c):
    return jnp.broadcast_to(x[:, c : c + 1], (8, 128))


def inverse_factor(read, write, one, beside):
    lane = lax.broadcasted_iota(jnp.int32, (8, 128), 1)
    strips = [read(k) for k in range(16)]
    for k in range(16):
        base = 8 * k
        inside = (lane >= base) & (lane < base + 8)
        cols = {q: [lane_of(strips[q], base + c) for c in range(8)] for q in range(k, 16)}
        for q in range(k + 1, 16):
            strips[q] = jnp.where(inside, 0.0, strips[q])
        rows = [jnp.where(inside, jnp.where(lane == base + s, 1.0, 0.0), row_of(strips[k], s)) for s in range(8)]
        own = [x * one for x in cols[k]]
        nxt = cols[k + 1] if k < 15 else None
        beside(k)
        scale, factor = [], {}
        for c in range(8):
            pivot = row_of(own[c], c)
            r = 1.0 / pivot
            scale.append(r)
            write(base + c, jnp.where(lane < base + 8, rows[c] * lax.rsqrt(pivot), 0.0)[:1, :])
            for s in range(c + 1, 8):
                f = row_of(own[c], s) * r
                factor[s, c] = f
                own[s] = own[s] - own[c] * f
                rows[s] = rows[s] - rows[c] * f
                if nxt is not None:
                    nxt[s] = nxt[s] - nxt[c] * f
            if nxt is not None:
                strips[k + 1] = strips[k + 1] - (nxt[c] * r) * rows[c]
        if k < 14:
            solved = [None] * 8
            for s in range(7, -1, -1):
                v = rows[s] * scale[s]
                for t in range(s + 1, 8):
                    v = v - factor[t, s] * solved[t]
                solved[s] = v
            for q in range(k + 2, 16):
                for c in range(8):
                    strips[q] = strips[q] - cols[q][c] * solved[c]


def rows_at(start, size):
    return pl.ds(pl.multiple_of(start, size), size)


def slab_kernel(where_ref, one_ref, *refs):
    piece_refs = refs[:5]
    ck_ref, cr_ref, f_ref, u_ref, hi_ref, lo_ref, a_ref, p_ref, acc_ref, d_ref, t_ref = refs[5:]
    z, y = where_ref[0] // 4, lax.rem(where_ref[0], 4)
    for ref, dy, slots in zip(piece_refs, (0, -1, 1, 2, 2), [range(8)] * 3 + [range(4), range(4, 8)]):
        for at, slot in enumerate(slots):
            to = 4 * lax.rem(z + (0, -1, 1, -2, 2, -3, 3, 4)[slot] + 8, 8) + lax.rem(y + dy + 4, 4)
            hi_ref[rows_at(to * 64, 64), 0:1152] = ref[64 * at : 64 * at + 64, :]
    for i in range(16):
        for j in range(i + 1):
            gap = i - j
            if gap <= 8:
                block = hi_ref[128 * i : 128 * i + 128, 128 * (8 - gap) : 128 * (9 - gap)]
            else:
                block = hi_ref[128 * j : 128 * j + 128, 128 * (gap - 8) : 128 * (gap - 7)].astype(F32).T.astype(BF16)
            a_ref[128 * i : 128 * i + 128, 128 * j : 128 * j + 128] = block
        if i % 2 == 0:
            a_ref[128 * i : 128 * i + 128, 128 * i + 128 : 128 * i + 256] = jnp.zeros((128, 128), BF16)
    a_ref[N : N + 512, :] = ck_ref[...]
    a_ref[N + 512 : N + 768, :] = cr_ref[...]

    def panel(p, carry):
        cols = rows_at(p * W, W)
        pairs = (12 - p) // 2

        @pl.when(p == 0)
        def _():
            def first(j, carry):
                rows = rows_at(j * 512, 512)
                p_ref[rows, :] = a_ref[rows, cols].astype(F32)
                return carry

            lax.fori_loop(0, 6, first, 0)

        @pl.when(p > 0)
        def _():
            old = rows_at((p - 1) * W, W)

            def update(j, carry):
                rows = pl.ds(pl.multiple_of((p + 2 * j) * W, W), 512)
                done = dot3((hi_ref[rows, old], lo_ref[rows, old]), (hi_ref[cols, old], lo_ref[cols, old]), 1, 1)
                before = jnp.where(p >= 2, acc_ref[rows, :], 0.0)
                p_ref[rows, :] = a_ref[rows, cols].astype(F32) - before - done
                return carry

            lax.fori_loop(0, pairs, update, 0)

        top = rows_at(p * W, 128)
        low = rows_at(p * W + 128, 128)
        ahead = rows_at(jnp.minimum(p + 1, PANELS - 1) * W, W)

        def half(h, place):
            @pl.when(h == 0)
            def _():
                d_ref[...] = p_ref[top, 0:128]

            @pl.when(h == 1)
            def _():
                below = dot3(split(p_ref[low, 0:128]), split(t_ref[0]), 1, 1)
                pair = split(below)
                d_ref[...] = p_ref[low, 128:256] - dot3(pair, pair, 1, 1)
                t_ref[2] = dot3(pair, split(t_ref[0]), 1, 0)

            def write(r, v):
                t_ref[h, r : r + 1, :] = v

            state = [place]

            def beside(k):
                if k >= SLOTS:
                    return
                t, i = state[0]
                idle = (i >= p) | (p >= PANELS - 1)
                rows = rows_at(jnp.where(idle, 11, t) * W, W)
                old = rows_at(jnp.where(idle, 0, i) * W, W)
                new = dot3((hi_ref[rows, old], lo_ref[rows, old]), (hi_ref[ahead, old], lo_ref[ahead, old]), 1, 1)
                acc_ref[rows, :] = jnp.where(i == 0, 0.0, acc_ref[rows, :]) + new
                wrap = t >= 10
                state[0] = (jnp.where(wrap, p + 1, t + 1), jnp.where(wrap, i + 1, i))

            inverse_factor(lambda k: d_ref[8 * k : 8 * k + 8, :], write, one_ref[...], beside)
            return state[0]

        lax.fori_loop(0, 2, half, (p + 1, 0))
        corner = split(t_ref[1])
        blocks = (split(t_ref[0]), split(-dot3(corner, split(t_ref[2]), 1, 0)), corner)
        zero = jnp.zeros((128, 128), BF16)
        t_pair = tuple(
            jnp.concatenate(
                [jnp.concatenate([blocks[0][e], zero], axis=1), jnp.concatenate([blocks[1][e], blocks[2][e]], axis=1)],
                axis=0,
            )
            for e in range(2)
        )
        for e in range(2):
            tp_ref = (hi_ref, lo_ref)[e]
            tp_ref[11 * W : 12 * W, 0:W] = t_pair[e]

        def scale(j, carry):
            rows = pl.ds(pl.multiple_of((p + 2 * j) * W, W), 512)
            new = split(
                dot3(split(p_ref[rows, :]), (hi_ref[11 * W : 12 * W, 0:W], lo_ref[11 * W : 12 * W, 0:W]), 1, 1)
            )
            hi_ref[rows, cols] = new[0]
            lo_ref[rows, cols] = new[1]
            return carry

        lax.fori_loop(0, pairs, scale, 0)
        return carry

    lax.fori_loop(0, PANELS, panel, 0)
    first = where_ref[0] * 64
    mine = rows_at(first, 64)
    keep = lax.broadcasted_iota(jnp.int32, (64, N), 1) <= lax.broadcasted_iota(jnp.int32, (64, N), 0) + first
    f_ref[...] = jnp.where(keep, hi_ref[mine, :].astype(F32) + lo_ref[mine, :].astype(F32), 0.0)
    u_ref[...] = dot(hi_ref[N + 512 : N + 768, :], hi_ref[N : N + 512, :], 1, 1).astype(BF16)


def finish_kernel(nd_ref, part_ref, out_ref):
    for q in range(16):
        left = 128 * (q % 2)
        lanes = slice(64 * (q // 2), 64 * (q // 2) + 64)
        pair = [part_ref[left + 64 * e : left + 64 * e + 64, lanes].astype(F32) for e in range(2)]
        cols = slice(128 * q, 128 * q + 128)
        out_ref[:, cols] = nd_ref[:, cols] - jnp.concatenate(pair, axis=1)


def vmem(count):
    return [pl.BlockSpec(memory_space=pltpu.VMEM)] * count


def smem():
    return [pl.BlockSpec(memory_space=pltpu.SMEM)]


def shape(dims, dtype):
    return jax.ShapeDtypeStruct(dims, dtype)


def cost(flops, moved):
    return pl.CostEstimate(flops=flops, bytes_accessed=moved, transcendentals=0)


def slab_call(*args):
    return pl.pallas_call(
        slab_kernel,
        out_shape=[shape((64, N), F32), shape((W, 512), BF16)],
        in_specs=smem() + vmem(8),
        out_specs=vmem(2),
        scratch_shapes=[
            pltpu.VMEM((12 * W, N), BF16),
            pltpu.VMEM((12 * W, N), BF16),
            pltpu.VMEM((12 * W, N), BF16),
            pltpu.VMEM((12 * W, W), F32),
            pltpu.VMEM((12 * W, W), F32),
            pltpu.VMEM((128, 128), F32),
            pltpu.VMEM((3, 128, 128), F32),
        ],
        compiler_params=pltpu.CompilerParams(vmem_limit_bytes=VMEM_LIMIT),
        cost_estimate=cost(60_000_000_000, 24_000_000),
    )(*args)


def shifted(value, by_z, by_y):
    pairs = [(4 * z + y, 4 * ((z + by_z) % 8) + (y + by_y) % 4) for z in range(8) for y in range(4)]
    return lax.ppermute(value, "blk", pairs)


def around(value, steps, by_z, by_y):
    up = down = value
    got = []
    for _ in range(steps - 1):
        up, down = shifted(up, by_z, by_y), shifted(down, -by_z, -by_y)
        got += [up, down]
    half = value.shape[0] // 2
    return got + [shifted(up[:half], by_z, by_y), shifted(down[half:], -by_z, -by_y)]


def local(schur, coupling, next_diag):
    index = lax.axis_index("blk")
    blk = index.astype(jnp.int32).reshape(1)
    start = 128 * ((index // 2 + 8) % 16)
    half = lax.dynamic_slice_in_dim(jnp.concatenate([schur, schur[:, :1024]], axis=1), start, 1152, 1)
    line = jnp.concatenate([half] + around(half, 4, 1, 0), axis=0)
    pieces = [line] + around(line, 2, 0, 1)
    lines_z = [[4 * z + y for z in range(8)] for y in range(4)]
    lines_y = [[4 * z + y for y in range(4)] for z in range(8)]
    c_rows = lax.all_gather(coupling, "blk", axis=0, tiled=True, axis_index_groups=lines_y)
    c_cols = lax.all_gather(coupling, "blk", axis=0, tiled=True, axis_index_groups=lines_z)
    mine, part = slab_call(blk, jnp.ones((8, 128), F32), *pieces, c_cols, c_rows)
    part = lax.all_to_all(part, "blk", 0, 0, axis_index_groups=lines_y, tiled=True)
    count = lax.axis_size("chain")
    part = lax.ppermute(part, "chain", [(s, s + 1) for s in range(count - 1)])
    fresh = pl.pallas_call(
        finish_kernel,
        out_shape=shape((64, N), F32),
        in_specs=vmem(2),
        out_specs=pl.BlockSpec(memory_space=pltpu.VMEM),
        cost_estimate=cost(200_000, 1_400_000),
    )(next_diag, part)
    return (mine, fresh)


def solution(mesh):
    placed = P(("chain", "blk"), None)
    return jax.shard_map(
        local, mesh=mesh, in_specs=(placed, placed, placed), out_specs=(placed, placed), check_vma=False
    )
```

```python
import jax
import jax.numpy as jnp
from jax import lax
from jax.experimental import pallas as pl
from jax.experimental.pallas import tpu as pltpu
from jax.sharding import PartitionSpec as P

F32, BF16 = jnp.float32, jnp.bfloat16
N = 2048
W = 256
PANELS = N // W
VMEM_LIMIT = 62 * 1024 * 1024


def split(x):
    hi = x.astype(BF16)
    return hi, (x - hi.astype(F32)).astype(BF16)


def dot(a, b, ca, cb):
    return lax.dot_general(a, b, (((ca,), (cb,)), ((), ())), preferred_element_type=F32)


def dot3(a, b, ca, cb):
    left = jnp.concatenate([a[0], a[0], a[1]], axis=ca)
    right = jnp.concatenate([b[0], b[1], b[0]], axis=cb)
    return dot(left, right, ca, cb)


def row_of(x, s):
    return jnp.broadcast_to(x[s : s + 1, :], (8, 128))


def lane_of(x, c):
    return jnp.broadcast_to(x[:, c : c + 1], (8, 128))


def inverse_factor(read, write, one, beside):
    lane = lax.broadcasted_iota(jnp.int32, (8, 128), 1)
    strips = [read(k) for k in range(16)]
    for k in range(16):
        base = 8 * k
        inside = (lane >= base) & (lane < base + 8)
        cols = {q: [lane_of(strips[q], base + c) for c in range(8)] for q in range(k, 16)}
        for q in range(k + 1, 16):
            strips[q] = jnp.where(inside, 0.0, strips[q])
        rows = [jnp.where(inside, jnp.where(lane == base + s, 1.0, 0.0), row_of(strips[k], s)) for s in range(8)]
        own = [x * one for x in cols[k]]
        nxt = cols[k + 1] if k < 15 else None
        beside(k)
        scale, factor = [], {}
        for c in range(8):
            pivot = row_of(own[c], c)
            r = 1.0 / pivot
            scale.append(r)
            write(base + c, jnp.where(lane < base + 8, rows[c] * lax.rsqrt(pivot), 0.0)[:1, :])
            for s in range(c + 1, 8):
                f = row_of(own[c], s) * r
                factor[s, c] = f
                own[s] = own[s] - own[c] * f
                rows[s] = rows[s] - rows[c] * f
                if nxt is not None:
                    nxt[s] = nxt[s] - nxt[c] * f
            if nxt is not None:
                strips[k + 1] = strips[k + 1] - (nxt[c] * r) * rows[c]
        if k < 14:
            solved = [None] * 8
            for s in range(7, -1, -1):
                v = rows[s] * scale[s]
                for t in range(s + 1, 8):
                    v = v - factor[t, s] * solved[t]
                solved[s] = v
            for q in range(k + 2, 16):
                for c in range(8):
                    strips[q] = strips[q] - cols[q][c] * solved[c]


def rows_at(start, size):
    return pl.ds(pl.multiple_of(start, size), size)


def slab_kernel(where_ref, one_ref, *refs):
    piece_refs = refs[:5]
    ck_ref, cr_ref, f_ref, u_ref, hi_ref, lo_ref, a_ref, acc_ref, x_ref, d_ref, t_ref, tp_ref = refs[5:]
    z, y = where_ref[0] // 4, lax.rem(where_ref[0], 4)
    for ref, dy, slots in zip(piece_refs, (0, -1, 1, 2, 2), [range(8)] * 3 + [range(4), range(4, 8)]):
        for at, slot in enumerate(slots):
            to = 4 * lax.rem(z + (0, -1, 1, -2, 2, -3, 3, 4)[slot] + 8, 8) + lax.rem(y + dy + 4, 4)
            hi_ref[rows_at(to * 64, 64), 0:1152] = ref[64 * at : 64 * at + 64, :]
    for i in range(16):
        for j in range(i + 1):
            gap = i - j
            if gap <= 8:
                block = hi_ref[128 * i : 128 * i + 128, 128 * (8 - gap) : 128 * (9 - gap)]
            else:
                block = hi_ref[128 * j : 128 * j + 128, 128 * (gap - 8) : 128 * (gap - 7)].astype(F32).T.astype(BF16)
            a_ref[128 * i : 128 * i + 128, 128 * j : 128 * j + 128] = block
        if i % 2 == 0:
            a_ref[128 * i : 128 * i + 128, 128 * i + 128 : 128 * i + 256] = jnp.zeros((128, 128), BF16)
    a_ref[N : N + 512, :] = ck_ref[...]
    a_ref[N + 512 : N + 768, :] = cr_ref[...]

    zeros = jnp.zeros((W, W), F32)

    def clear(j, carry):
        acc_ref[rows_at(j * W, W), :] = zeros
        return carry

    lax.fori_loop(0, 26, clear, 0)

    def known(rows, cols):
        return hi_ref[rows, cols], lo_ref[rows, cols]

    def tile(t):
        return rows_at(t * W, W)

    def panel(p, carry):
        cols = tile(p)
        prev = tile(jnp.maximum(p - 1, 0))
        mine, other = 12 * lax.rem(p, 2), 12 * lax.rem(p + 1, 2)
        x_ref[0:W, :] = a_ref[cols, cols].astype(F32) - acc_ref[24 * W : 25 * W, :]
        acc_ref[24 * W : 25 * W, :] = zeros

        @pl.when(p > 0)
        def _():
            pair = known(cols, prev)
            x_ref[0:W, :] -= dot3(pair, pair, 1, 1)

        def half(h, place):
            @pl.when(h == 0)
            def _():
                d_ref[...] = x_ref[0:128, 0:128]

            @pl.when(h == 1)
            def _():
                below = dot3(split(x_ref[128:256, 0:128]), split(t_ref[0]), 1, 1)
                pair = split(below)
                d_ref[...] = x_ref[128:256, 128:256] - dot3(pair, pair, 1, 1)
                t_ref[2] = dot3(pair, split(t_ref[0]), 1, 0)

            def write(r, v):
                t_ref[h, r : r + 1, :] = v

            state = [place]

            def past(k):
                t, n = state[0]
                diagonal = (h == 1) & (k < p)
                idle = (n >= p) | (p < 2)
                late = n == 0
                left = jnp.where(diagonal, p + 1, jnp.where(idle, 11, t))
                right = jnp.where(diagonal, p + 1, jnp.where(late, jnp.maximum(p - 1, 0), p))
                old = tile(jnp.where(diagonal, k, jnp.where(late, jnp.maximum(p - 2, 0), jnp.where(idle, 0, n - 1))))
                to = tile(jnp.where(diagonal, 24, jnp.where(idle, 25, jnp.where(late, other, mine) + t)))
                acc_ref[to, :] += dot3(known(tile(left), old), known(tile(right), old), 1, 1)
                wrap = t >= 10
                after = (jnp.where(wrap, p + 1, t + 1), jnp.where(wrap, n + 1, n))
                state[0] = tuple(jnp.where(diagonal, a, b) for a, b in zip(state[0], after))

            def finish(j):
                t = p + 1 + 5 * h + j
                idle = (t > 10) | (p < 1)
                rows = tile(jnp.where(idle, 11, t))
                at = tile(jnp.where(idle, 25, other + t))
                left = a_ref[rows, prev].astype(F32) - acc_ref[at, :]
                acc_ref[at, :] = zeros
                hi_ref[rows, prev], lo_ref[rows, prev] = split(dot3(split(left), (tp_ref[0], tp_ref[1]), 1, 1))

            def beside(k):
                for e in range(2 * k, min(2 * k + 2, 15)):
                    past(e)
                if 8 <= k < 13:
                    finish(k - 8)

            inverse_factor(lambda k: d_ref[8 * k : 8 * k + 8, :], write, one_ref[...], beside)
            return state[0]

        lax.fori_loop(0, 2, half, (p + 1, 0))
        corner = split(t_ref[1])
        blocks = (split(t_ref[0]), split(-dot3(corner, split(t_ref[2]), 1, 0)), corner)
        for e in range(2):
            tp_ref[e, 0:128, 0:128] = blocks[0][e]
            tp_ref[e, 0:128, 128:256] = jnp.zeros((128, 128), BF16)
            tp_ref[e, 128:256, 0:128] = blocks[1][e]
            tp_ref[e, 128:256, 128:256] = blocks[2][e]
        next_rows = tile(p + 1)
        at = tile(mine + p + 1)
        x_ref[W : 2 * W, :] = a_ref[next_rows, cols].astype(F32) - acc_ref[at, :]
        acc_ref[at, :] = zeros

        @pl.when(p > 0)
        def _():
            x_ref[W : 2 * W, :] -= dot3(known(next_rows, prev), known(cols, prev), 1, 1)

        both = pl.ds(pl.multiple_of(p * W, W), 2 * W)
        hi_ref[both, cols], lo_ref[both, cols] = split(dot3(split(x_ref[...]), (tp_ref[0], tp_ref[1]), 1, 1))
        return carry

    lax.fori_loop(0, PANELS, panel, 0)
    tail, end = slice(9 * W, 11 * W), slice(7 * W, 8 * W)
    left = a_ref[tail, end].astype(F32) - acc_ref[21 * W : 23 * W, :]
    left = left - dot3(known(tail, slice(6 * W, 7 * W)), known(end, slice(6 * W, 7 * W)), 1, 1)
    hi_ref[tail, end], lo_ref[tail, end] = split(dot3(split(left), (tp_ref[0], tp_ref[1]), 1, 1))
    first = where_ref[0] * 64
    mine = rows_at(first, 64)
    keep = lax.broadcasted_iota(jnp.int32, (64, N), 1) <= lax.broadcasted_iota(jnp.int32, (64, N), 0) + first
    f_ref[...] = jnp.where(keep, hi_ref[mine, :].astype(F32) + lo_ref[mine, :].astype(F32), 0.0)
    u_ref[...] = dot(hi_ref[N + 512 : N + 768, :], hi_ref[N : N + 512, :], 1, 1).astype(BF16)


def finish_kernel(nd_ref, part_ref, out_ref):
    for q in range(16):
        left = 128 * (q % 2)
        lanes = slice(64 * (q // 2), 64 * (q // 2) + 64)
        pair = [part_ref[left + 64 * e : left + 64 * e + 64, lanes].astype(F32) for e in range(2)]
        cols = slice(128 * q, 128 * q + 128)
        out_ref[:, cols] = nd_ref[:, cols] - jnp.concatenate(pair, axis=1)


def vmem(count):
    return [pl.BlockSpec(memory_space=pltpu.VMEM)] * count


def smem():
    return [pl.BlockSpec(memory_space=pltpu.SMEM)]


def shape(dims, dtype):
    return jax.ShapeDtypeStruct(dims, dtype)


def cost(flops, moved):
    return pl.CostEstimate(flops=flops, bytes_accessed=moved, transcendentals=0)


def slab_call(*args):
    return pl.pallas_call(
        slab_kernel,
        out_shape=[shape((64, N), F32), shape((W, 512), BF16)],
        in_specs=smem() + vmem(8),
        out_specs=vmem(2),
        scratch_shapes=[
            pltpu.VMEM((12 * W, N), BF16),
            pltpu.VMEM((12 * W, N), BF16),
            pltpu.VMEM((12 * W, N), BF16),
            pltpu.VMEM((26 * W, W), F32),
            pltpu.VMEM((2 * W, W), F32),
            pltpu.VMEM((128, 128), F32),
            pltpu.VMEM((3, 128, 128), F32),
            pltpu.VMEM((2, W, W), BF16),
        ],
        compiler_params=pltpu.CompilerParams(vmem_limit_bytes=VMEM_LIMIT),
        cost_estimate=cost(60_000_000_000, 24_000_000),
    )(*args)


def shifted(value, by_z, by_y):
    pairs = [(4 * z + y, 4 * ((z + by_z) % 8) + (y + by_y) % 4) for z in range(8) for y in range(4)]
    return lax.ppermute(value, "blk", pairs)


def around(value, steps, by_z, by_y):
    up = down = value
    got = []
    for _ in range(steps - 1):
        up, down = shifted(up, by_z, by_y), shifted(down, -by_z, -by_y)
        got += [up, down]
    half = value.shape[0] // 2
    return got + [shifted(up[:half], by_z, by_y), shifted(down[half:], -by_z, -by_y)]


def local(schur, coupling, next_diag):
    index = lax.axis_index("blk")
    blk = index.astype(jnp.int32).reshape(1)
    start = 128 * ((index // 2 + 8) % 16)
    half = lax.dynamic_slice_in_dim(jnp.concatenate([schur, schur[:, :1024]], axis=1), start, 1152, 1)
    line = jnp.concatenate([half] + around(half, 4, 1, 0), axis=0)
    pieces = [line] + around(line, 2, 0, 1)
    lines_z = [[4 * z + y for z in range(8)] for y in range(4)]
    lines_y = [[4 * z + y for y in range(4)] for z in range(8)]
    c_rows = lax.all_gather(coupling, "blk", axis=0, tiled=True, axis_index_groups=lines_y)
    c_cols = lax.all_gather(coupling, "blk", axis=0, tiled=True, axis_index_groups=lines_z)
    mine, part = slab_call(blk, jnp.ones((8, 128), F32), *pieces, c_cols, c_rows)
    part = lax.all_to_all(part, "blk", 0, 0, axis_index_groups=lines_y, tiled=True)
    count = lax.axis_size("chain")
    part = lax.ppermute(part, "chain", [(s, s + 1) for s in range(count - 1)])
    fresh = pl.pallas_call(
        finish_kernel,
        out_shape=shape((64, N), F32),
        in_specs=vmem(2),
        out_specs=pl.BlockSpec(memory_space=pltpu.VMEM),
        cost_estimate=cost(200_000, 1_400_000),
    )(next_diag, part)
    return (mine, fresh)


def solution(mesh):
    placed = P(("chain", "blk"), None)
    return jax.shard_map(
        local, mesh=mesh, in_specs=(placed, placed, placed), out_specs=(placed, placed), check_vma=False
    )
```

```python
import functools

import jax
import jax.numpy as jnp
from jax import lax
from jax.experimental import pallas as pl
from jax.experimental.pallas import tpu as pltpu
from jax.sharding import PartitionSpec as P

F32, BF16 = jnp.float32, jnp.bfloat16
N = 2048
W = 256
PANELS = N // W
VMEM_LIMIT = 62 * 1024 * 1024


def split(x):
    hi = x.astype(BF16)
    return hi, (x - hi.astype(F32)).astype(BF16)


def dot(a, b, ca, cb):
    return lax.dot_general(a, b, (((ca,), (cb,)), ((), ())), preferred_element_type=F32)


def dot3(a, b, ca, cb):
    left = jnp.concatenate([a[0], a[0], a[1]], axis=ca)
    right = jnp.concatenate([b[0], b[1], b[0]], axis=cb)
    return dot(left, right, ca, cb)


def row_of(x, s):
    return jnp.broadcast_to(x[s : s + 1, :], (8, 128))


def lane_of(x, c):
    return jnp.broadcast_to(x[:, c : c + 1], (8, 128))


def inverse_factor(read, write, one, beside):
    lane = lax.broadcasted_iota(jnp.int32, (8, 128), 1)
    strips = [read(k) for k in range(16)]
    for k in range(16):
        base = 8 * k
        inside = (lane >= base) & (lane < base + 8)
        cols = {q: [lane_of(strips[q], base + c) for c in range(8)] for q in range(k, 16)}
        for q in range(k + 1, 16):
            strips[q] = jnp.where(inside, 0.0, strips[q])
        rows = [jnp.where(inside, jnp.where(lane == base + s, 1.0, 0.0), row_of(strips[k], s)) for s in range(8)]
        own = [x * one for x in cols[k]]
        nxt = cols[k + 1] if k < 15 else None
        beside(k)
        scale, factor = [], {}
        for c in range(8):
            pivot = row_of(own[c], c)
            r = 1.0 / pivot
            scale.append(r)
            write(base + c, jnp.where(lane < base + 8, rows[c] * lax.rsqrt(pivot), 0.0)[:1, :])
            for s in range(c + 1, 8):
                f = row_of(own[c], s) * r
                factor[s, c] = f
                own[s] = own[s] - own[c] * f
                rows[s] = rows[s] - rows[c] * f
                if nxt is not None:
                    nxt[s] = nxt[s] - nxt[c] * f
            if nxt is not None:
                strips[k + 1] = strips[k + 1] - (nxt[c] * r) * rows[c]
        if k < 14:
            solved = [None] * 8
            for s in range(7, -1, -1):
                v = rows[s] * scale[s]
                for t in range(s + 1, 8):
                    v = v - factor[t, s] * solved[t]
                solved[s] = v
            for q in range(k + 2, 16):
                for c in range(8):
                    strips[q] = strips[q] - cols[q][c] * solved[c]


def rows_at(start, size):
    return pl.ds(pl.multiple_of(start, size), size)


def slab_kernel(where_ref, one_ref, *refs):
    piece_refs = refs[:5]
    ck_ref, cr_ref, f_ref, u_ref, hi_ref, lo_ref, a_ref, acc_ref, x_ref, d_ref, t_ref, tp_ref = refs[5:]
    z, y = where_ref[0] // 4, lax.rem(where_ref[0], 4)
    for ref, dy, slots in zip(piece_refs, (0, -1, 1, 2, 2), [range(8)] * 3 + [range(4), range(4, 8)]):
        for at, slot in enumerate(slots):
            to = 4 * lax.rem(z + (0, -1, 1, -2, 2, -3, 3, 4)[slot] + 8, 8) + lax.rem(y + dy + 4, 4)
            hi_ref[rows_at(to * 64, 64), 0:1152] = ref[64 * at : 64 * at + 64, :]
    for i in range(16):
        for j in range(i + 1):
            gap = i - j
            if gap <= 8:
                block = hi_ref[128 * i : 128 * i + 128, 128 * (8 - gap) : 128 * (9 - gap)]
            else:
                block = hi_ref[128 * j : 128 * j + 128, 128 * (gap - 8) : 128 * (gap - 7)].astype(F32).T.astype(BF16)
            a_ref[128 * i : 128 * i + 128, 128 * j : 128 * j + 128] = block
        if i % 2 == 0:
            a_ref[128 * i : 128 * i + 128, 128 * i + 128 : 128 * i + 256] = jnp.zeros((128, 128), BF16)
    a_ref[N : N + 512, :] = ck_ref[...]
    a_ref[N + 512 : N + 768, :] = cr_ref[...]

    zeros = jnp.zeros((W, W), F32)

    def clear(j, carry):
        acc_ref[rows_at(j * W, W), :] = zeros
        return carry

    lax.fori_loop(0, 26, clear, 0)

    def known(rows, cols):
        return hi_ref[rows, cols], lo_ref[rows, cols]

    def tile(t):
        return rows_at(t * W, W)

    def panel(p, carry, early):
        cols = tile(p)
        prev = tile(jnp.maximum(p - 1, 0))
        mine, other = 12 * lax.rem(p, 2), 12 * lax.rem(p + 1, 2)
        x_ref[0:W, :] = a_ref[cols, cols].astype(F32) - acc_ref[24 * W : 25 * W, :]
        acc_ref[24 * W : 25 * W, :] = zeros

        @pl.when(p > 0)
        def _():
            pair = known(cols, prev)
            x_ref[0:W, :] -= dot3(pair, pair, 1, 1)

        def half(h, place):
            @pl.when(h == 0)
            def _():
                d_ref[...] = x_ref[0:128, 0:128]

            @pl.when(h == 1)
            def _():
                below = dot3(split(x_ref[128:256, 0:128]), split(t_ref[0]), 1, 1)
                pair = split(below)
                d_ref[...] = x_ref[128:256, 128:256] - dot3(pair, pair, 1, 1)
                t_ref[2] = dot3(pair, split(t_ref[0]), 1, 0)

            def write(r, v):
                t_ref[h, r : r + 1, :] = v

            state = [place]

            def past(k):
                t, n = state[0]
                diagonal = (h == 1) & (k < p)
                idle = (n >= p) | (p < 2)
                late = n == 0
                left = jnp.where(diagonal, p + 1, jnp.where(idle, 11, t))
                right = jnp.where(diagonal, p + 1, jnp.where(late, jnp.maximum(p - 1, 0), p))
                old = tile(jnp.where(diagonal, k, jnp.where(late, jnp.maximum(p - 2, 0), jnp.where(idle, 0, n - 1))))
                to = tile(jnp.where(diagonal, 24, jnp.where(idle, 25, jnp.where(late, other, mine) + t)))
                acc_ref[to, :] += dot3(known(tile(left), old), known(tile(right), old), 1, 1)
                wrap = t >= 10
                after = (jnp.where(wrap, p + 1, t + 1), jnp.where(wrap, n + 1, n))
                state[0] = tuple(jnp.where(diagonal, a, b) for a, b in zip(state[0], after))

            def finish(j):
                t = p + 1 + 5 * h + j
                idle = (t > 10) | (p < 1)
                rows = tile(jnp.where(idle, 11, t))
                at = tile(jnp.where(idle, 25, other + t))
                left = a_ref[rows, prev].astype(F32) - acc_ref[at, :]
                acc_ref[at, :] = zeros
                hi_ref[rows, prev], lo_ref[rows, prev] = split(dot3(split(left), (tp_ref[0], tp_ref[1]), 1, 1))

            def beside(k):
                for e in range(2 * k, min(2 * k + 2, 1 if early else 15)):
                    past(e)
                if 8 <= k < 13:
                    finish(k - 8)

            inverse_factor(lambda k: d_ref[8 * k : 8 * k + 8, :], write, one_ref[...], beside)
            return state[0]

        lax.fori_loop(0, 2, half, (p + 1, 0))
        corner = split(t_ref[1])
        blocks = (split(t_ref[0]), split(-dot3(corner, split(t_ref[2]), 1, 0)), corner)
        for e in range(2):
            tp_ref[e, 0:128, 0:128] = blocks[0][e]
            tp_ref[e, 0:128, 128:256] = jnp.zeros((128, 128), BF16)
            tp_ref[e, 128:256, 0:128] = blocks[1][e]
            tp_ref[e, 128:256, 128:256] = blocks[2][e]
        next_rows = tile(p + 1)
        at = tile(mine + p + 1)
        x_ref[W : 2 * W, :] = a_ref[next_rows, cols].astype(F32) - acc_ref[at, :]
        acc_ref[at, :] = zeros

        @pl.when(p > 0)
        def _():
            x_ref[W : 2 * W, :] -= dot3(known(next_rows, prev), known(cols, prev), 1, 1)

        both = pl.ds(pl.multiple_of(p * W, W), 2 * W)
        hi_ref[both, cols], lo_ref[both, cols] = split(dot3(split(x_ref[...]), (tp_ref[0], tp_ref[1]), 1, 1))
        return carry

    lax.fori_loop(0, 2, functools.partial(panel, early=True), 0)
    lax.fori_loop(2, PANELS, functools.partial(panel, early=False), 0)
    tail, end = slice(9 * W, 11 * W), slice(7 * W, 8 * W)
    left = a_ref[tail, end].astype(F32) - acc_ref[21 * W : 23 * W, :]
    left = left - dot3(known(tail, slice(6 * W, 7 * W)), known(end, slice(6 * W, 7 * W)), 1, 1)
    hi_ref[tail, end], lo_ref[tail, end] = split(dot3(split(left), (tp_ref[0], tp_ref[1]), 1, 1))
    first = where_ref[0] * 64
    mine = rows_at(first, 64)
    keep = lax.broadcasted_iota(jnp.int32, (64, N), 1) <= lax.broadcasted_iota(jnp.int32, (64, N), 0) + first
    f_ref[...] = jnp.where(keep, hi_ref[mine, :].astype(F32) + lo_ref[mine, :].astype(F32), 0.0)
    u_ref[...] = dot(hi_ref[N + 512 : N + 768, :], hi_ref[N : N + 512, :], 1, 1).astype(BF16)


def finish_kernel(nd_ref, part_ref, out_ref):
    for q in range(16):
        left = 128 * (q % 2)
        lanes = slice(64 * (q // 2), 64 * (q // 2) + 64)
        pair = [part_ref[left + 64 * e : left + 64 * e + 64, lanes].astype(F32) for e in range(2)]
        cols = slice(128 * q, 128 * q + 128)
        out_ref[:, cols] = nd_ref[:, cols] - jnp.concatenate(pair, axis=1)


def vmem(count):
    return [pl.BlockSpec(memory_space=pltpu.VMEM)] * count


def smem():
    return [pl.BlockSpec(memory_space=pltpu.SMEM)]


def shape(dims, dtype):
    return jax.ShapeDtypeStruct(dims, dtype)


def cost(flops, moved):
    return pl.CostEstimate(flops=flops, bytes_accessed=moved, transcendentals=0)


def slab_call(*args):
    return pl.pallas_call(
        slab_kernel,
        out_shape=[shape((64, N), F32), shape((W, 512), BF16)],
        in_specs=smem() + vmem(8),
        out_specs=vmem(2),
        scratch_shapes=[
            pltpu.VMEM((12 * W, N), BF16),
            pltpu.VMEM((12 * W, N), BF16),
            pltpu.VMEM((12 * W, N), BF16),
            pltpu.VMEM((26 * W, W), F32),
            pltpu.VMEM((2 * W, W), F32),
            pltpu.VMEM((128, 128), F32),
            pltpu.VMEM((3, 128, 128), F32),
            pltpu.VMEM((2, W, W), BF16),
        ],
        compiler_params=pltpu.CompilerParams(vmem_limit_bytes=VMEM_LIMIT),
        cost_estimate=cost(60_000_000_000, 24_000_000),
    )(*args)


def shifted(value, by_z, by_y):
    pairs = [(4 * z + y, 4 * ((z + by_z) % 8) + (y + by_y) % 4) for z in range(8) for y in range(4)]
    return lax.ppermute(value, "blk", pairs)


def around(value, steps, by_z, by_y):
    up = down = value
    got = []
    for _ in range(steps - 1):
        up, down = shifted(up, by_z, by_y), shifted(down, -by_z, -by_y)
        got += [up, down]
    half = value.shape[0] // 2
    return got + [shifted(up[:half], by_z, by_y), shifted(down[half:], -by_z, -by_y)]


def local(schur, coupling, next_diag):
    index = lax.axis_index("blk")
    blk = index.astype(jnp.int32).reshape(1)
    start = 128 * ((index // 2 + 8) % 16)
    half = lax.dynamic_slice_in_dim(jnp.concatenate([schur, schur[:, :1024]], axis=1), start, 1152, 1)
    line = jnp.concatenate([half] + around(half, 4, 1, 0), axis=0)
    pieces = [line] + around(line, 2, 0, 1)
    lines_z = [[4 * z + y for z in range(8)] for y in range(4)]
    lines_y = [[4 * z + y for y in range(4)] for z in range(8)]
    c_rows = lax.all_gather(coupling, "blk", axis=0, tiled=True, axis_index_groups=lines_y)
    c_cols = lax.all_gather(coupling, "blk", axis=0, tiled=True, axis_index_groups=lines_z)
    mine, part = slab_call(blk, jnp.ones((8, 128), F32), *pieces, c_cols, c_rows)
    part = lax.all_to_all(part, "blk", 0, 0, axis_index_groups=lines_y, tiled=True)
    count = lax.axis_size("chain")
    part = lax.ppermute(part, "chain", [(s, s + 1) for s in range(count - 1)])
    fresh = pl.pallas_call(
        finish_kernel,
        out_shape=shape((64, N), F32),
        in_specs=vmem(2),
        out_specs=pl.BlockSpec(memory_space=pltpu.VMEM),
        cost_estimate=cost(200_000, 1_400_000),
    )(next_diag, part)
    return (mine, fresh)


def solution(mesh):
    placed = P(("chain", "blk"), None)
    return jax.shard_map(
        local, mesh=mesh, in_specs=(placed, placed, placed), out_specs=(placed, placed), check_vma=False
    )
```
